32 devices in a mesh: blk: 8 (over y, x, core), rel: 4 (over z).
Axes of the slice: x: 2, y: 2, z: 4, core: 2. Of those that a mesh axis runs over, the one named last changes fastest.
Arguments:
- features: bfloat16 [4096, 512], P(('blk', 'rel')), may hold values from -6 to 6
- adjacency: int32 [6, 128, 4, 1024], P(None, 'blk', 'rel'), may hold values from -2147483648 to 2147483646, as said below
- tile_mask: int32 [6, 32, 8, 4], P(None, 'blk', None, 'rel'), may hold values from 0 to 1
- bases: bfloat16 [512, 8, 512], P('rel'), may hold values from -0.25 to 0.25
- coefficients: float32 [6, 8], replicated, may hold values from -2 to 2
- self_weight: bfloat16 [512, 512], P('rel'), may hold values from -0.25 to 0.25
Outputs:
- updated: bfloat16 [4096, 512], P(('blk', 'rel'))
The draws below stay inside these ranges and needn't reach their ends.
Inputs may be any that keep to these rules, and one draw needn't show every extreme that they name: `adjacency`: each word holds 32 edge bits, bit t for destination node 32 * word index + t.
All inputs are finite; a program needn't handle non-finite values.
Results may differ from the reference program's by a relative error of at most 0.0058.
Values may be sent and summed in bfloat16 or wider, within the bound.
No kernel may reach another device: no remote copies, remote signals or barrier semaphores. Data moves between devices by JAX's collectives and lax.ppermute only.
A program may use at most 64 MiB of HBM per device.

```python
import jax
import jax.numpy as jnp
from jax import lax

D = 512
RELS = 6
BASES = 8
NODE_DEV = 512
NODES = 4096
SUB = 128
N_BLK = 8
N_REL = 4


def draw_adjacency(key, part):
    shape = (RELS, NODES // 32, N_REL, N_BLK * SUB)
    first = jax.random.randint(jax.random.fold_in(key, 31), shape, -2147483648, 2147483647, dtype=jnp.int32)
    second = jax.random.randint(jax.random.fold_in(key, 37), shape, -2147483648, 2147483647, dtype=jnp.int32)
    third = jax.random.randint(jax.random.fold_in(key, 41), shape, -2147483648, 2147483647, dtype=jnp.int32)
    return jnp.bitwise_and(jnp.bitwise_and(first, second), third)


def draw_tile_mask(key, part):
    rate_key = jax.random.fold_in(key, 11)
    dense_key = jax.random.fold_in(key, 13)
    pick_key = jax.random.fold_in(key, 17)
    value_key = jax.random.fold_in(key, 23)
    sparse_rates = jax.random.randint(rate_key, (RELS, NODES // 128, 1, 1), 2, 26)
    dense_rates = jax.random.randint(dense_key, (RELS, NODES // 128, 1, 1), 30, 61)
    picked = jax.random.randint(pick_key, (RELS, NODES // 128, 1, 1), 0, 8) == 0
    rates = jnp.where(picked, dense_rates, sparse_rates)
    values = jax.random.randint(value_key, (RELS, NODES // 128, N_BLK, N_REL), 0, 100)
    return (values < rates).astype(jnp.int32)


def shard_levels(key, shape, pieces, low, high):
    def one(dim, parts):
        draws = jax.random.uniform(jax.random.fold_in(jax.random.fold_in(key, 6), dim), (parts,), jnp.float32, low / len(pieces), high / len(pieces))
        return jnp.repeat(jnp.exp(draws), shape[dim] // parts).reshape((-1,) + (1,) * (len(shape) - dim - 1))

    loudness = one(*pieces[0])
    for cut in pieces[1:]:
        loudness = loudness * one(*cut)
    return loudness


def normal_values(rng, dims, deviation, limit, cuts=(), kind=jnp.bfloat16):
    level = shard_levels(rng, dims, cuts, -0.22, 0.18) if cuts else 1.0
    result = jax.random.normal(rng, dims, jnp.float32) * deviation * level
    return jnp.minimum(jnp.maximum(result, -limit), limit).astype(kind)


def setup_inputs(seed: int = 0) -> dict:
    arg_keys = jax.random.split(jax.random.key(seed), 7)
    return {
        "features": normal_values(arg_keys[0], (NODES, D), 1.0, 6.0, ((0, 32),)),
        "adjacency": draw_adjacency(jax.random.fold_in(arg_keys[6], 71), 0),
        "tile_mask": draw_tile_mask(jax.random.fold_in(arg_keys[6], 71), 0),
        "bases": normal_values(arg_keys[3], (D, BASES, D), D ** -0.5, 0.25, ((0, 4),)),
        "coefficients": normal_values(arg_keys[4], (RELS, BASES), 0.35, 2.0, (), jnp.float32),
        "self_weight": normal_values(arg_keys[5], (D, D), D ** -0.5, 0.25, ((0, 4),)),
    }


def expand_edges(packed, tile_flags):
    shifts = jnp.arange(32, dtype=jnp.int32)
    edge_bits = jnp.bitwise_and(jnp.right_shift(packed[:, :, None, :], shifts[None, None, :, None]), 1)
    edge_bits = edge_bits.reshape(packed.shape[0], packed.shape[1] * 32, packed.shape[2])
    tile_rows = jnp.repeat(tile_flags, 128, axis=1)
    return edge_bits * tile_rows

def reference(features, adjacency, tile_mask, bases, coefficients, self_weight):
    relations = adjacency.shape[0]
    width = features.shape[1]
    rel_weight = jnp.einsum('rb,ibj->irj', coefficients.astype(jnp.float32), bases.astype(jnp.float32), precision=lax.Precision.HIGHEST).astype(jnp.bfloat16)
    projected = jnp.dot(features, rel_weight.reshape(width, relations * width), preferred_element_type=jnp.float32)
    projected = projected.astype(jnp.bfloat16).reshape(NODES, relations, width)
    reordered = adjacency.reshape(relations, NODES // 32, N_REL, N_BLK, SUB)
    reordered = jnp.transpose(reordered, (0, 1, 3, 2, 4))
    packed_all = reordered.reshape(relations, NODES // 32, N_BLK, NODE_DEV)
    flags_all = jnp.repeat(tile_mask, SUB, axis=3)

    def one_block(carry, block):
        running, degree = carry
        packed = lax.dynamic_index_in_dim(packed_all, block, 2, keepdims=False)
        flags = lax.dynamic_index_in_dim(flags_all, block, 2, keepdims=False)
        edges = expand_edges(packed, flags).astype(jnp.float32)
        values = lax.dynamic_slice_in_dim(projected, (block * NODE_DEV).astype(jnp.int32), NODE_DEV, 0).astype(jnp.float32)
        running = running + jnp.einsum('rns,srd->nd', edges, values)
        degree = degree + lax.optimization_barrier(jnp.sum(edges, axis=(0, 2)))
        return ((running, degree), None)
    start = (jnp.zeros((NODES, width), jnp.float32), jnp.zeros((NODES,), jnp.float32))
    (message, degree), _ = lax.scan(one_block, start, jnp.arange(N_BLK, dtype=jnp.int32))
    own = jnp.dot(features, self_weight, preferred_element_type=jnp.float32)
    return jax.nn.relu(own + message * lax.rsqrt(1.0 + degree)[:, None]).astype(jnp.bfloat16)
```

```python
import jax
import jax.numpy as jnp
from jax import lax
from jax.sharding import PartitionSpec as P


def expand_edges(packed, tile_flags):
    shifts = jnp.arange(32, dtype=jnp.int32)
    edge_bits = jnp.bitwise_and(
        jnp.right_shift(packed[:, :, None, :], shifts[None, None, :, None]), 1
    )
    edge_bits = edge_bits.reshape(packed.shape[0], packed.shape[1] * 32, packed.shape[2])
    tile_rows = jnp.repeat(tile_flags, 128, axis=1)
    return edge_bits * tile_rows


def from_shift(value, axis, size, shift):
    return lax.ppermute(value, axis, [(i, (i + shift) % size) for i in range(size)])


def gather_pairs(value, size, group):
    b = lax.axis_index("blk")
    out = []
    for t in range(size // group):
        got = value if t == 0 else from_shift(value, "blk", size, group * t)
        source = (b - group * t) % size
        out.append((source, got))
        if group == 2:
            other = lax.ppermute(got, "blk", [(i, i ^ 1) for i in range(size)])
            out.append((source ^ 1, other))
    return out


def make(blks, rels):
    group = 2 if blks % 2 == 0 else 1

    def shards(features, adjacency, tile_mask, bases, coefficients, self_weight):
        relations = adjacency.shape[0]
        words = adjacency.shape[1]
        blocks = tile_mask.shape[2]
        sub_rows = features.shape[0]
        width = features.shape[1]
        rows = bases.shape[0]
        piece = rows // blks
        cols = (relations + 1) * width
        b = lax.axis_index("blk")
        j = lax.axis_index("rel")

        def weights(some_bases, some_self):
            made = jnp.einsum(
                "rb,ibj->irj", coefficients, some_bases.astype(jnp.float32),
                precision=lax.Precision.HIGHEST,
            ).astype(jnp.bfloat16)
            return jnp.concatenate([made.reshape(-1, relations * width), some_self], axis=1)

        mine = weights(
            lax.dynamic_slice_in_dim(bases, b * piece, piece, 0),
            lax.dynamic_slice_in_dim(self_weight, b * piece, piece, 0),
        )
        others = jnp.stack([from_shift(mine, "rel", rels, s) for s in range(1, rels)])

        split = features.reshape(sub_rows, rels, rows)
        ordered = jnp.concatenate(
            [lax.dynamic_index_in_dim(split, (j - s) % rels, 1, keepdims=False) for s in range(rels)],
            axis=1,
        )
        portion = jnp.zeros((blks, sub_rows, width), features.dtype)
        for source, got in gather_pairs(ordered, blks, group):
            portion = lax.dynamic_update_index_in_dim(portion, got, source, 0)
        portion = portion.reshape(blks * sub_rows, width)

        packed_all = adjacency.reshape(relations, words, blocks * sub_rows)
        flags_all = jnp.repeat(
            tile_mask.reshape(relations, tile_mask.shape[1], blocks), sub_rows, axis=2
        )
        edges = expand_edges(packed_all, flags_all)
        degree = jnp.sum(edges, axis=(0, 2)).astype(jnp.float32).reshape(rels, sub_rows)
        edges = edges.astype(jnp.bfloat16)

        def scatter_sum(parts):
            total = lax.dynamic_index_in_dim(parts, j, 0, keepdims=False).astype(jnp.float32)
            for s in range(1, rels):
                part = lax.dynamic_index_in_dim(parts, (j + s) % rels, 0, keepdims=False)
                total = total + from_shift(part, "rel", rels, s).astype(jnp.float32)
            return total

        degree = scatter_sum(degree)

        weight_rest = jnp.zeros((rels - 1, blks, piece, cols), jnp.bfloat16)
        for source, got in gather_pairs(others, blks, group):
            weight_rest = lax.dynamic_update_index_in_dim(weight_rest, got, source, 1)
        weight_all = jnp.concatenate(
            [weights(bases, self_weight), weight_rest.reshape((rels - 1) * rows, cols)], axis=0
        )
        values = jnp.dot(
            portion, weight_all[:, : relations * width], preferred_element_type=jnp.float32
        ).astype(jnp.bfloat16)
        values = values.reshape(portion.shape[0], relations, width)
        message = jnp.einsum("rns,srd->nd", edges, values, preferred_element_type=jnp.float32)
        message = scatter_sum(message.astype(jnp.bfloat16).reshape(rels, sub_rows, width))
        own = jnp.dot(
            ordered, weight_all[:, relations * width :], preferred_element_type=jnp.float32
        )
        return jax.nn.relu(own + message * lax.rsqrt(1.0 + degree)[:, None]).astype(jnp.bfloat16)

    return shards


def solution(mesh):
    placed = (
        P(("blk", "rel"), None),
        P(None, "blk", "rel", None),
        P(None, "blk", None, "rel"),
        P("rel", None, None),
        P(),
        P("rel", None),
    )
    return jax.shard_map(
        make(mesh.shape["blk"], mesh.shape["rel"]), mesh=mesh, in_specs=placed,
        out_specs=P(("blk", "rel"), None), check_vma=False,
    )
```

```python
import jax
import jax.numpy as jnp
from jax import lax
from jax.experimental import pallas as pl
from jax.experimental.pallas import tpu as pltpu
from jax.sharding import PartitionSpec as P


def expand_edges(packed, tile_flags):
    shifts = jnp.arange(32, dtype=jnp.int32)
    edge_bits = jnp.bitwise_and(
        jnp.right_shift(packed[:, :, None, :], shifts[None, None, :, None]), 1
    )
    edge_bits = edge_bits.reshape(packed.shape[0], packed.shape[1] * 32, packed.shape[2])
    tile_rows = jnp.repeat(tile_flags, 128, axis=1)
    return edge_bits * tile_rows


def from_shift(value, axis, size, shift):
    return lax.ppermute(value, axis, [(i, (i + shift) % size) for i in range(size)])


def gather_pairs(value, size, group):
    b = lax.axis_index("blk")
    out = []
    for t in range(size // group):
        got = value if t == 0 else from_shift(value, "blk", size, group * t)
        source = (b - group * t) % size
        out.append((source, got))
        if group == 2:
            other = lax.ppermute(got, "blk", [(i, i ^ 1) for i in range(size)])
            out.append((source ^ 1, other))
    return out


def message_kernel(portion, weight_own, weight_rest, edges, out, total):
    r = pl.program_id(0)
    weight = jnp.concatenate([weight_own[...], weight_rest[...]], axis=0)
    values = jnp.dot(portion[...], weight, preferred_element_type=jnp.float32).astype(jnp.bfloat16)
    part = jnp.dot(edges[0], values, preferred_element_type=jnp.float32)

    @pl.when(r == 0)
    def _():
        total[...] = part

    @pl.when(r > 0)
    def _():
        total[...] += part

    @pl.when(r == pl.num_programs(0) - 1)
    def _():
        out[...] = total[...].astype(out.dtype)


def messages(portion, weight_own, weight_rest, edges):
    relations, targets, sources = edges.shape
    width = portion.shape[1]
    return pl.pallas_call(
        message_kernel,
        grid=(relations,),
        in_specs=[
            pl.BlockSpec((sources, width), lambda r: (0, 0)),
            pl.BlockSpec((weight_own.shape[0], width), lambda r: (0, r)),
            pl.BlockSpec((weight_rest.shape[0], width), lambda r: (0, r)),
            pl.BlockSpec((1, targets, sources), lambda r: (r, 0, 0)),
        ],
        out_specs=pl.BlockSpec((targets, width), lambda r: (0, 0)),
        out_shape=jax.ShapeDtypeStruct((targets, width), jnp.bfloat16),
        scratch_shapes=[pltpu.VMEM((targets, width), jnp.float32)],
        compiler_params=pltpu.CompilerParams(dimension_semantics=("arbitrary",)),
    )(portion, weight_own, weight_rest, edges)


def make(blks, rels):
    group = 2 if blks % 2 == 0 else 1

    def shards(features, adjacency, tile_mask, bases, coefficients, self_weight):
        relations = adjacency.shape[0]
        words = adjacency.shape[1]
        blocks = tile_mask.shape[2]
        sub_rows = features.shape[0]
        width = features.shape[1]
        rows = bases.shape[0]
        piece = rows // blks
        cols = (relations + 1) * width
        b = lax.axis_index("blk")
        j = lax.axis_index("rel")

        def weights(some_bases, some_self):
            made = jnp.einsum(
                "rb,ibj->irj", coefficients, some_bases.astype(jnp.float32),
                precision=lax.Precision.HIGHEST,
            ).astype(jnp.bfloat16)
            return jnp.concatenate([made.reshape(-1, relations * width), some_self], axis=1)

        mine = weights(
            lax.dynamic_slice_in_dim(bases, b * piece, piece, 0),
            lax.dynamic_slice_in_dim(self_weight, b * piece, piece, 0),
        )
        others = jnp.stack([from_shift(mine, "rel", rels, s) for s in range(1, rels)])

        split = features.reshape(sub_rows, rels, rows)
        ordered = jnp.concatenate(
            [lax.dynamic_index_in_dim(split, (j - s) % rels, 1, keepdims=False) for s in range(rels)],
            axis=1,
        )
        portion = jnp.zeros((blks, sub_rows, width), features.dtype)
        for source, got in gather_pairs(ordered, blks, group):
            portion = lax.dynamic_update_index_in_dim(portion, got, source, 0)
        portion = portion.reshape(blks * sub_rows, width)

        others, adjacency = lax.optimization_barrier((others, adjacency))
        weight_own = weights(bases, self_weight)[:, : relations * width]
        packed_all = adjacency.reshape(relations, words, blocks * sub_rows)
        flags_all = jnp.repeat(
            tile_mask.reshape(relations, tile_mask.shape[1], blocks), sub_rows, axis=2
        )
        edges = expand_edges(packed_all, flags_all)
        degree = jnp.sum(edges, axis=(0, 2)).astype(jnp.float32).reshape(rels, sub_rows)
        edges = edges.astype(jnp.bfloat16)

        def scatter_sum(parts):
            total = lax.dynamic_index_in_dim(parts, j, 0, keepdims=False).astype(jnp.float32)
            for s in range(1, rels):
                part = lax.dynamic_index_in_dim(parts, (j + s) % rels, 0, keepdims=False)
                total = total + from_shift(part, "rel", rels, s).astype(jnp.float32)
            return total

        degree = scatter_sum(degree)

        weight_rest = jnp.zeros((rels - 1, blks, piece, cols), jnp.bfloat16)
        for source, got in gather_pairs(others, blks, group):
            weight_rest = lax.dynamic_update_index_in_dim(weight_rest, got, source, 1)
        weight_rest = weight_rest.reshape((rels - 1) * rows, cols)
        message = messages(portion, weight_own, weight_rest, edges)
        message = scatter_sum(message.reshape(rels, sub_rows, width))
        self_all = jnp.concatenate([self_weight, weight_rest[:, relations * width :]], axis=0)
        own = jnp.dot(ordered, self_all, preferred_element_type=jnp.float32)
        return jax.nn.relu(own + message * lax.rsqrt(1.0 + degree)[:, None]).astype(jnp.bfloat16)

    return shards


def solution(mesh):
    placed = (
        P(("blk", "rel"), None),
        P(None, "blk", "rel", None),
        P(None, "blk", None, "rel"),
        P("rel", None, None),
        P(),
        P("rel", None),
    )
    return jax.shard_map(
        make(mesh.shape["blk"], mesh.shape["rel"]), mesh=mesh, in_specs=placed,
        out_specs=P(("blk", "rel"), None), check_vma=False,
    )
```

```python
import jax
import jax.numpy as jnp
from jax import lax
from jax.experimental import pallas as pl
from jax.experimental.pallas import tpu as pltpu
from jax.sharding import PartitionSpec as P


def expand_edges(packed, tile_flags):
    shifts = jnp.arange(32, dtype=jnp.int32)
    edge_bits = jnp.bitwise_and(
        jnp.right_shift(packed[:, :, None, :], shifts[None, None, :, None]), 1
    )
    edge_bits = edge_bits.reshape(packed.shape[0], packed.shape[1] * 32, packed.shape[2])
    tile_rows = jnp.repeat(tile_flags, 128, axis=1)
    return edge_bits * tile_rows


def from_shift(value, axis, size, shift):
    return lax.ppermute(value, axis, [(i, (i + shift) % size) for i in range(size)])


def gather_pairs(value, size, group):
    b = lax.axis_index("blk")
    out = []
    for t in range(size // group):
        got = value if t == 0 else from_shift(value, "blk", size, group * t)
        source = (b - group * t) % size
        out.append((source, got))
        if group == 2:
            other = lax.ppermute(got, "blk", [(i, i ^ 1) for i in range(size)])
            out.append((source ^ 1, other))
    return out


def messages(sources, ordered, features, weight_own, pieces, edges):
    relations, targets, nodes = edges.shape
    sub_rows, width = ordered.shape
    rows = weight_own.shape[0]
    shifts, piece = pieces[0].shape[:2]
    count, parts = len(features), len(pieces)

    def kernel(source, own_features, *refs):
        feature_refs, refs = refs[:count], refs[count:]
        own_ref, refs = refs[0], refs[1:]
        piece_refs, refs = refs[:parts], refs[parts:]
        edge_ref, out, own_out, portion, weight, total = refs
        step = pl.program_id(0)

        weight[:rows] = own_ref[...]
        for k, ref in enumerate(piece_refs):
            for s in range(shifts):
                place = (s + 1) * rows + (source[k] * piece if parts > 1 else 0)
                weight[pl.ds(pl.multiple_of(place, piece), piece)] = ref[s]

        @pl.when(step == 0)
        def _():
            for k, ref in enumerate(feature_refs):
                place = pl.multiple_of(source[k] * sub_rows, sub_rows)
                portion[pl.ds(place, sub_rows)] = ref[...]
            own_out[...] = jnp.dot(
                own_features[...], weight[...], preferred_element_type=jnp.float32
            )
            total[...] = jnp.zeros_like(total)

        @pl.when(step > 0)
        def _():
            values = jnp.dot(portion[...], weight[...], preferred_element_type=jnp.float32)
            total[...] += jnp.dot(
                edge_ref[0], values.astype(jnp.bfloat16), preferred_element_type=jnp.float32
            )

        @pl.when(step == pl.num_programs(0) - 1)
        def _():
            out[...] = total[...].astype(out.dtype)

    def column(step):
        return (step + relations) % (relations + 1)

    whole = pl.BlockSpec((sub_rows, width), lambda r, _: (0, 0))
    return pl.pallas_call(
        kernel,
        grid_spec=pltpu.PrefetchScalarGridSpec(
            num_scalar_prefetch=1,
            grid=(relations + 1,),
            in_specs=[whole] * (count + 1)
            + [pl.BlockSpec((rows, width), lambda r, _: (0, column(r)))]
            + [pl.BlockSpec((shifts, piece, width), lambda r, _: (0, 0, column(r)))] * parts
            + [pl.BlockSpec((1, targets, nodes), lambda r, _: (jnp.maximum(r - 1, 0), 0, 0))],
            out_specs=[pl.BlockSpec((targets, width), lambda r, _: (0, 0)), whole],
            scratch_shapes=[
                pltpu.VMEM((nodes, width), jnp.bfloat16),
                pltpu.VMEM((rows * (shifts + 1), width), jnp.bfloat16),
                pltpu.VMEM((targets, width), jnp.float32),
            ],
        ),
        out_shape=[
            jax.ShapeDtypeStruct((targets, width), jnp.bfloat16),
            jax.ShapeDtypeStruct((sub_rows, width), jnp.float32),
        ],
        compiler_params=pltpu.CompilerParams(dimension_semantics=("arbitrary",)),
    )(sources, ordered, *features, weight_own, *pieces, edges)


def make(blks, rels):
    group = 2 if blks % 2 == 0 else 1

    def shards(features, adjacency, tile_mask, bases, coefficients, self_weight):
        relations = adjacency.shape[0]
        words = adjacency.shape[1]
        blocks = tile_mask.shape[2]
        sub_rows = features.shape[0]
        width = features.shape[1]
        rows = bases.shape[0]
        piece = rows // blks
        cols = (relations + 1) * width
        b = lax.axis_index("blk")
        j = lax.axis_index("rel")

        def weights(some_bases, some_self):
            made = jnp.einsum(
                "rb,ibj->irj", coefficients, some_bases.astype(jnp.float32),
                precision=lax.Precision.HIGHEST,
            ).astype(jnp.bfloat16)
            return jnp.concatenate([made.reshape(-1, relations * width), some_self], axis=1)

        mine = weights(
            lax.dynamic_slice_in_dim(bases, b * piece, piece, 0),
            lax.dynamic_slice_in_dim(self_weight, b * piece, piece, 0),
        )
        others = jnp.stack([from_shift(mine, "rel", rels, s) for s in range(1, rels)])

        split = features.reshape(sub_rows, rels, rows)
        ordered = jnp.concatenate(
            [lax.dynamic_index_in_dim(split, (j - s) % rels, 1, keepdims=False) for s in range(rels)],
            axis=1,
        )
        gathered = gather_pairs(ordered, blks, group)

        others, adjacency = lax.optimization_barrier((others, adjacency))
        weight_own = weights(bases, self_weight)
        packed_all = adjacency.reshape(relations, words, blocks * sub_rows)
        flags_all = jnp.repeat(
            tile_mask.reshape(relations, tile_mask.shape[1], blocks), sub_rows, axis=2
        )
        edges = expand_edges(packed_all, flags_all)
        degree = jnp.sum(edges, axis=(0, 2)).astype(jnp.float32).reshape(rels, sub_rows)
        edges = edges.astype(jnp.bfloat16)

        def scatter_sum(parts):
            total = lax.dynamic_index_in_dim(parts, j, 0, keepdims=False).astype(jnp.float32)
            for s in range(1, rels):
                part = lax.dynamic_index_in_dim(parts, (j + s) % rels, 0, keepdims=False)
                total = total + from_shift(part, "rel", rels, s).astype(jnp.float32)
            return total

        degree = scatter_sum(degree)

        shared = gather_pairs(others, blks, group)
        pieces = [got for _, got in shared]
        if piece % 16:
            rest = jnp.zeros((rels - 1, blks, piece, cols), jnp.bfloat16)
            for source, got in shared:
                rest = lax.dynamic_update_index_in_dim(rest, got, source, 1)
            pieces = [rest.reshape(rels - 1, rows, cols)]
        message, own = messages(
            jnp.stack([source for source, _ in gathered]).astype(jnp.int32),
            ordered, [got for _, got in gathered], weight_own, pieces, edges,
        )
        message = scatter_sum(message.reshape(rels, sub_rows, width))
        return jax.nn.relu(own + message * lax.rsqrt(1.0 + degree)[:, None]).astype(jnp.bfloat16)

    return shards


def solution(mesh):
    placed = (
        P(("blk", "rel"), None),
        P(None, "blk", "rel", None),
        P(None, "blk", None, "rel"),
        P("rel", None, None),
        P(),
        P("rel", None),
    )
    return jax.shard_map(
        make(mesh.shape["blk"], mesh.shape["rel"]), mesh=mesh, in_specs=placed,
        out_specs=P(("blk", "rel"), None), check_vma=False,
    )
```

```python
import jax
import jax.numpy as jnp
from jax import lax
from jax.experimental import pallas as pl
from jax.experimental.pallas import tpu as pltpu
from jax.sharding import PartitionSpec as P


def expand_edges(packed, tile_flags):
    shifts = jnp.arange(32, dtype=jnp.int32)
    edge_bits = jnp.bitwise_and(
        jnp.right_shift(packed[:, :, None, :], shifts[None, None, :, None]), 1
    )
    edge_bits = edge_bits.reshape(packed.shape[0], packed.shape[1] * 32, packed.shape[2])
    tile_rows = jnp.repeat(tile_flags, 128, axis=1)
    return edge_bits * tile_rows


def from_shift(value, axis, size, shift):
    return lax.ppermute(value, axis, [(i, (i + shift) % size) for i in range(size)])


def gather_pairs(value, size, group, meanwhile=()):
    b = lax.axis_index("blk")
    came = [value] + [from_shift(value, "blk", size, group * t) for t in range(1, size // group)]
    if meanwhile:
        far, meanwhile = lax.optimization_barrier((came[1:], meanwhile))
        came[1:] = far
    out = []
    for t, got in enumerate(came):
        source = (b - group * t) % size
        out.append((source, got))
        if group == 2:
            other = lax.ppermute(got, "blk", [(i, i ^ 1) for i in range(size)])
            out.append((source ^ 1, other))
    return out, meanwhile


def messages(sources, ordered, features, weight_own, pieces, edges):
    relations, targets, nodes = edges.shape
    sub_rows, width = ordered.shape
    rows = weight_own.shape[0]
    shifts, piece = pieces[0].shape[:2]
    count, parts = len(features), len(pieces)

    def kernel(source, own_features, *refs):
        feature_refs, refs = refs[:count], refs[count:]
        own_ref, refs = refs[0], refs[1:]
        piece_refs, refs = refs[:parts], refs[parts:]
        edge_ref, out, own_out, portion, weight, total = refs
        step = pl.program_id(0)

        weight[:rows] = own_ref[...]
        for k, ref in enumerate(piece_refs):
            for s in range(shifts):
                place = (s + 1) * rows + (source[k] * piece if parts > 1 else 0)
                weight[pl.ds(pl.multiple_of(place, piece), piece)] = ref[s]

        @pl.when(step == 0)
        def _():
            for k, ref in enumerate(feature_refs):
                place = pl.multiple_of(source[k] * sub_rows, sub_rows)
                portion[pl.ds(place, sub_rows)] = ref[...]
            own_out[...] = jnp.dot(
                own_features[...], weight[...], preferred_element_type=jnp.float32
            )
            total[...] = jnp.zeros_like(total)

        @pl.when(step > 0)
        def _():
            values = jnp.dot(portion[...], weight[...], preferred_element_type=jnp.float32)
            total[...] += jnp.dot(
                edge_ref[0], values.astype(jnp.bfloat16), preferred_element_type=jnp.float32
            )

        @pl.when(step == pl.num_programs(0) - 1)
        def _():
            out[...] = total[...].astype(out.dtype)

    def column(step):
        return (step + relations) % (relations + 1)

    whole = pl.BlockSpec((sub_rows, width), lambda r, _: (0, 0))
    return pl.pallas_call(
        kernel,
        grid_spec=pltpu.PrefetchScalarGridSpec(
            num_scalar_prefetch=1,
            grid=(relations + 1,),
            in_specs=[whole] * (count + 1)
            + [pl.BlockSpec((rows, width), lambda r, _: (0, column(r)))]
            + [pl.BlockSpec((shifts, piece, width), lambda r, _: (0, 0, column(r)))] * parts
            + [pl.BlockSpec((1, targets, nodes), lambda r, _: (jnp.maximum(r - 1, 0), 0, 0))],
            out_specs=[pl.BlockSpec((targets, width), lambda r, _: (0, 0)), whole],
            scratch_shapes=[
                pltpu.VMEM((nodes, width), jnp.bfloat16),
                pltpu.VMEM((rows * (shifts + 1), width), jnp.bfloat16),
                pltpu.VMEM((targets, width), jnp.float32),
            ],
        ),
        out_shape=[
            jax.ShapeDtypeStruct((targets, width), jnp.bfloat16),
            jax.ShapeDtypeStruct((sub_rows, width), jnp.float32),
        ],
        compiler_params=pltpu.CompilerParams(dimension_semantics=("arbitrary",)),
    )(sources, ordered, *features, weight_own, *pieces, edges)


def make(blks, rels):
    group = 2 if blks % 2 == 0 else 1

    def shards(features, adjacency, tile_mask, bases, coefficients, self_weight):
        relations = adjacency.shape[0]
        words = adjacency.shape[1]
        blocks = tile_mask.shape[2]
        sub_rows = features.shape[0]
        width = features.shape[1]
        rows = bases.shape[0]
        piece = rows // blks
        cols = (relations + 1) * width
        b = lax.axis_index("blk")
        j = lax.axis_index("rel")

        def weights(some_bases, some_self):
            made = jnp.einsum(
                "rb,ibj->irj", coefficients, some_bases.astype(jnp.float32),
                precision=lax.Precision.HIGHEST,
            ).astype(jnp.bfloat16)
            return jnp.concatenate([made.reshape(-1, relations * width), some_self], axis=1)

        mine = weights(
            lax.dynamic_slice_in_dim(bases, b * piece, piece, 0),
            lax.dynamic_slice_in_dim(self_weight, b * piece, piece, 0),
        )
        others = jnp.stack([from_shift(mine, "rel", rels, s) for s in range(1, rels)])

        split = features.reshape(sub_rows, rels, rows)
        ordered = jnp.concatenate(
            [lax.dynamic_index_in_dim(split, (j - s) % rels, 1, keepdims=False) for s in range(rels)],
            axis=1,
        )
        gathered, _ = gather_pairs(ordered, blks, group)

        others, adjacency = lax.optimization_barrier((others, adjacency))
        weight_own = weights(bases, self_weight)
        packed_all = adjacency.reshape(relations, words, blocks * sub_rows)
        flags_all = jnp.repeat(
            tile_mask.reshape(relations, tile_mask.shape[1], blocks), sub_rows, axis=2
        )
        edges = expand_edges(packed_all, flags_all)
        degree = jnp.sum(edges, axis=(0, 2)).astype(jnp.float32).reshape(rels, sub_rows)
        edges = edges.astype(jnp.bfloat16)

        def scatter_sum(parts):
            total = lax.dynamic_index_in_dim(parts, j, 0, keepdims=False).astype(jnp.float32)
            for s in range(1, rels):
                part = lax.dynamic_index_in_dim(parts, (j + s) % rels, 0, keepdims=False)
                total = total + from_shift(part, "rel", rels, s).astype(jnp.float32)
            return total

        shared, (edges, degree) = gather_pairs(others, blks, group, (edges, degree))
        degree = scatter_sum(degree)
        pieces = [got for _, got in shared]
        if piece % 16:
            rest = jnp.zeros((rels - 1, blks, piece, cols), jnp.bfloat16)
            for source, got in shared:
                rest = lax.dynamic_update_index_in_dim(rest, got, source, 1)
            pieces = [rest.reshape(rels - 1, rows, cols)]
        message, own = messages(
            jnp.stack([source for source, _ in gathered]).astype(jnp.int32),
            ordered, [got for _, got in gathered], weight_own, pieces, edges,
        )
        message = scatter_sum(message.reshape(rels, sub_rows, width))
        return jax.nn.relu(own + message * lax.rsqrt(1.0 + degree)[:, None]).astype(jnp.bfloat16)

    return shards


def solution(mesh):
    placed = (
        P(("blk", "rel"), None),
        P(None, "blk", "rel", None),
        P(None, "blk", None, "rel"),
        P("rel", None, None),
        P(),
        P("rel", None),
    )
    return jax.shard_map(
        make(mesh.shape["blk"], mesh.shape["rel"]), mesh=mesh, in_specs=placed,
        out_specs=P(("blk", "rel"), None), check_vma=False,
    )
```

```python
import jax
import jax.numpy as jnp
from jax import lax
from jax.experimental import pallas as pl
from jax.experimental.pallas import tpu as pltpu
from jax.sharding import PartitionSpec as P


def expand_edges(packed, tile_flags):
    shifts = jnp.arange(32, dtype=jnp.int32)
    edge_bits = jnp.bitwise_and(
        jnp.right_shift(packed[:, :, None, :], shifts[None, None, :, None]), 1
    )
    edge_bits = edge_bits.reshape(packed.shape[0], packed.shape[1] * 32, packed.shape[2])
    tile_rows = jnp.repeat(tile_flags, 128, axis=1)
    return edge_bits * tile_rows


def from_shift(value, axis, size, shift):
    return lax.ppermute(value, axis, [(i, (i + shift) % size) for i in range(size)])


def gather_pairs(value, size, group, meanwhile=()):
    b = lax.axis_index("blk")
    came = [value] + [from_shift(value, "blk", size, group * t) for t in range(1, size // group)]
    if meanwhile:
        far, meanwhile = lax.optimization_barrier((came[1:], meanwhile))
        came[1:] = far
    out = []
    for t, got in enumerate(came):
        source = (b - group * t) % size
        out.append((source, got))
        if group == 2:
            other = lax.ppermute(got, "blk", [(i, i ^ 1) for i in range(size)])
            out.append((source ^ 1, other))
    return out, meanwhile


def messages(sources, ordered, features, weight_own, pieces, edges):
    relations, targets, nodes = edges.shape
    sub_rows, width = ordered.shape
    rows = weight_own.shape[0]
    shifts, piece = pieces[0].shape[:2]
    count, parts = len(features), len(pieces)

    def kernel(source, own_features, *refs):
        feature_refs, refs = refs[:count], refs[count:]
        own_ref, refs = refs[0], refs[1:]
        piece_refs, refs = refs[:parts], refs[parts:]
        edge_ref, out, own_out, portion, weight, total = refs
        step = pl.program_id(0)

        weight[:rows] = own_ref[...]
        for k, ref in enumerate(piece_refs):
            for s in range(shifts):
                place = (s + 1) * rows + (source[k] * piece if parts > 1 else 0)
                weight[pl.ds(pl.multiple_of(place, piece), piece)] = ref[s]

        @pl.when(step == 0)
        def _():
            for k, ref in enumerate(feature_refs):
                place = pl.multiple_of(source[k] * sub_rows, sub_rows)
                portion[pl.ds(place, sub_rows)] = ref[...]
            own_out[...] = jnp.dot(
                own_features[...], weight[...], preferred_element_type=jnp.float32
            )
            total[...] = jnp.zeros_like(total)

        @pl.when(step > 0)
        def _():
            values = jnp.dot(portion[...], weight[...], preferred_element_type=jnp.float32)
            total[...] += jnp.dot(
                edge_ref[0], values.astype(jnp.bfloat16), preferred_element_type=jnp.float32
            )

        @pl.when(step == pl.num_programs(0) - 1)
        def _():
            out[...] = total[...].astype(out.dtype)

    def column(step):
        return (step + relations) % (relations + 1)

    whole = pl.BlockSpec((sub_rows, width), lambda r, _: (0, 0))
    return pl.pallas_call(
        kernel,
        grid_spec=pltpu.PrefetchScalarGridSpec(
            num_scalar_prefetch=1,
            grid=(relations + 1,),
            in_specs=[whole] * (count + 1)
            + [pl.BlockSpec((rows, width), lambda r, _: (0, column(r)))]
            + [pl.BlockSpec((shifts, piece, width), lambda r, _: (0, 0, column(r)))] * parts
            + [pl.BlockSpec((1, targets, nodes), lambda r, _: (jnp.maximum(r - 1, 0), 0, 0))],
            out_specs=[pl.BlockSpec((targets, width), lambda r, _: (0, 0)), whole],
            scratch_shapes=[
                pltpu.VMEM((nodes, width), jnp.bfloat16),
                pltpu.VMEM((rows * (shifts + 1), width), jnp.bfloat16),
                pltpu.VMEM((targets, width), jnp.float32),
            ],
        ),
        out_shape=[
            jax.ShapeDtypeStruct((targets, width), jnp.bfloat16),
            jax.ShapeDtypeStruct((sub_rows, width), jnp.float32),
        ],
        compiler_params=pltpu.CompilerParams(dimension_semantics=("arbitrary",)),
    )(sources, ordered, *features, weight_own, *pieces, edges)


def make(blks, rels):
    group = 2 if blks % 2 == 0 else 1

    def shards(features, adjacency, tile_mask, bases, coefficients, self_weight):
        relations = adjacency.shape[0]
        words = adjacency.shape[1]
        blocks = tile_mask.shape[2]
        sub_rows = features.shape[0]
        width = features.shape[1]
        rows = bases.shape[0]
        piece = rows // blks
        cols = (relations + 1) * width
        b = lax.axis_index("blk")
        j = lax.axis_index("rel")

        def weights(some_bases, some_self):
            made = jnp.einsum(
                "rb,ibj->irj", coefficients, some_bases.astype(jnp.float32),
                precision=lax.Precision.HIGHEST,
            ).astype(jnp.bfloat16)
            return jnp.concatenate([made.reshape(-1, relations * width), some_self], axis=1)

        mine = weights(
            lax.dynamic_slice_in_dim(bases, b * piece, piece, 0),
            lax.dynamic_slice_in_dim(self_weight, b * piece, piece, 0),
        )
        others = jnp.stack([from_shift(mine, "rel", rels, s) for s in range(1, rels)])

        split = features.reshape(sub_rows, rels, rows)
        ordered = jnp.concatenate(
            [lax.dynamic_index_in_dim(split, (j - s) % rels, 1, keepdims=False) for s in range(rels)],
            axis=1,
        )
        gathered, _ = gather_pairs(ordered, blks, group)

        others, adjacency = lax.optimization_barrier((others, adjacency))
        weight_own = weights(bases, self_weight)
        packed_all = adjacency.reshape(relations, words, blocks * sub_rows)
        flags_all = jnp.repeat(
            tile_mask.reshape(relations, tile_mask.shape[1], blocks), sub_rows, axis=2
        )
        edges = expand_edges(packed_all, flags_all)
        degree = jnp.sum(edges, axis=(0, 2)).astype(jnp.float32).reshape(rels, sub_rows)
        edges = edges.astype(jnp.bfloat16)

        def scatter_sum(parts):
            total = lax.dynamic_index_in_dim(parts, j, 0, keepdims=False).astype(jnp.float32)
            for s in range(1, rels):
                part = lax.dynamic_index_in_dim(parts, (j + s) % rels, 0, keepdims=False)
                total = total + from_shift(part, "rel", rels, s).astype(jnp.float32)
            return total

        shared, (edges, degree, weight_own) = gather_pairs(
            others, blks, group, (edges, scatter_sum(degree), weight_own)
        )
        pieces = [got for _, got in shared]
        if piece % 16:
            rest = jnp.zeros((rels - 1, blks, piece, cols), jnp.bfloat16)
            for source, got in shared:
                rest = lax.dynamic_update_index_in_dim(rest, got, source, 1)
            pieces = [rest.reshape(rels - 1, rows, cols)]
        message, own = messages(
            jnp.stack([source for source, _ in gathered]).astype(jnp.int32),
            ordered, [got for _, got in gathered], weight_own, pieces, edges,
        )
        message = scatter_sum(message.reshape(rels, sub_rows, width))
        return jax.nn.relu(own + message * lax.rsqrt(1.0 + degree)[:, None]).astype(jnp.bfloat16)

    return shards


def solution(mesh):
    placed = (
        P(("blk", "rel"), None),
        P(None, "blk", "rel", None),
        P(None, "blk", None, "rel"),
        P("rel", None, None),
        P(),
        P("rel", None),
    )
    return jax.shard_map(
        make(mesh.shape["blk"], mesh.shape["rel"]), mesh=mesh, in_specs=placed,
        out_specs=P(("blk", "rel"), None), check_vma=False,
    )
```

```python
import jax
import jax.numpy as jnp
from jax import lax
from jax.experimental import pallas as pl
from jax.experimental.pallas import tpu as pltpu
from jax.sharding import PartitionSpec as P


def expand_edges(packed, tile_flags):
    shifts = jnp.arange(32, dtype=jnp.int32)
    edge_bits = jnp.bitwise_and(
        jnp.right_shift(packed[:, :, None, :], shifts[None, None, :, None]), 1
    )
    edge_bits = edge_bits.reshape(packed.shape[0], packed.shape[1] * 32, packed.shape[2])
    tile_rows = jnp.repeat(tile_flags, 128, axis=1)
    return edge_bits * tile_rows


def from_shift(value, axis, size, shift):
    return lax.ppermute(value, axis, [(i, (i + shift) % size) for i in range(size)])


def gather_pairs(value, size, group, meanwhile=()):
    b = lax.axis_index("blk")
    came = [value] + [from_shift(value, "blk", size, group * t) for t in range(1, size // group)]
    if meanwhile:
        far, meanwhile = lax.optimization_barrier((came[1:], meanwhile))
        came[1:] = far
    out = []
    for t, got in enumerate(came):
        source = (b - group * t) % size
        out.append((source, got))
        if group == 2:
            other = lax.ppermute(got, "blk", [(i, i ^ 1) for i in range(size)])
            out.append((source ^ 1, other))
    return out, meanwhile


def messages(sources, ordered, features, weight_own, pieces, edges):
    relations, targets, nodes = edges.shape
    sub_rows, width = ordered.shape
    rows = weight_own.shape[0]
    shifts, piece = pieces[0].shape[:2]
    count, parts = len(features), len(pieces)

    def kernel(source, own_features, *refs):
        feature_refs, refs = refs[:count], refs[count:]
        own_ref, refs = refs[0], refs[1:]
        piece_refs, refs = refs[:parts], refs[parts:]
        edge_ref, out, own_out, portion, weight, total = refs
        step = pl.program_id(0)

        weight[:rows] = own_ref[...]
        for k, ref in enumerate(piece_refs):
            for s in range(shifts):
                place = (s + 1) * rows + (source[k] * piece if parts > 1 else 0)
                weight[pl.ds(pl.multiple_of(place, piece), piece)] = ref[s]

        @pl.when(step == 0)
        def _():
            for k, ref in enumerate(feature_refs):
                place = pl.multiple_of(source[k] * sub_rows, sub_rows)
                portion[pl.ds(place, sub_rows)] = ref[...]
            own_out[...] = jnp.dot(
                own_features[...], weight[...], preferred_element_type=jnp.float32
            )
            total[...] = jnp.zeros_like(total)

        @pl.when(step > 0)
        def _():
            values = jnp.dot(portion[...], weight[...], preferred_element_type=jnp.float32)
            total[...] += jnp.dot(
                edge_ref[0], values.astype(jnp.bfloat16), preferred_element_type=jnp.float32
            )

        @pl.when(step == pl.num_programs(0) - 1)
        def _():
            out[...] = total[...].astype(out.dtype)

    def column(step):
        return (step + relations) % (relations + 1)

    whole = pl.BlockSpec((sub_rows, width), lambda r, _: (0, 0))
    return pl.pallas_call(
        kernel,
        grid_spec=pltpu.PrefetchScalarGridSpec(
            num_scalar_prefetch=1,
            grid=(relations + 1,),
            in_specs=[whole] * (count + 1)
            + [pl.BlockSpec((rows, width), lambda r, _: (0, column(r)))]
            + [pl.BlockSpec((shifts, piece, width), lambda r, _: (0, 0, column(r)))] * parts
            + [pl.BlockSpec((1, targets, nodes), lambda r, _: (jnp.maximum(r - 1, 0), 0, 0))],
            out_specs=[pl.BlockSpec((targets, width), lambda r, _: (0, 0)), whole],
            scratch_shapes=[
                pltpu.VMEM((nodes, width), jnp.bfloat16),
                pltpu.VMEM((rows * (shifts + 1), width), jnp.bfloat16),
                pltpu.VMEM((targets, width), jnp.float32),
            ],
        ),
        out_shape=[
            jax.ShapeDtypeStruct((targets, width), jnp.bfloat16),
            jax.ShapeDtypeStruct((sub_rows, width), jnp.float32),
        ],
        compiler_params=pltpu.CompilerParams(dimension_semantics=("arbitrary",)),
    )(sources, ordered, *features, weight_own, *pieces, edges)


def make(blks, rels):
    group = 2 if blks % 2 == 0 else 1

    def shards(features, adjacency, tile_mask, bases, coefficients, self_weight):
        relations = adjacency.shape[0]
        words = adjacency.shape[1]
        blocks = tile_mask.shape[2]
        sub_rows = features.shape[0]
        width = features.shape[1]
        rows = bases.shape[0]
        piece = rows // blks
        cols = (relations + 1) * width
        b = lax.axis_index("blk")
        j = lax.axis_index("rel")

        def weights(some_bases, some_self):
            made = jnp.einsum(
                "rb,ibj->irj", coefficients, some_bases.astype(jnp.float32),
                precision=lax.Precision.HIGHEST,
            ).astype(jnp.bfloat16)
            return jnp.concatenate([made.reshape(-1, relations * width), some_self], axis=1)

        mine = weights(
            lax.dynamic_slice_in_dim(bases, b * piece, piece, 0),
            lax.dynamic_slice_in_dim(self_weight, b * piece, piece, 0),
        )
        others = jnp.stack([from_shift(mine, "rel", rels, s) for s in range(1, rels)])

        split = features.reshape(sub_rows, rels, rows)
        ordered = jnp.concatenate(
            [lax.dynamic_index_in_dim(split, (j - s) % rels, 1, keepdims=False) for s in range(rels)],
            axis=1,
        )
        gathered, _ = gather_pairs(ordered, blks, group)

        others, adjacency = lax.optimization_barrier((others, adjacency))
        weight_own = weights(bases, self_weight)
        packed_all = adjacency.reshape(relations, words, blocks * sub_rows)
        flags_all = jnp.repeat(
            tile_mask.reshape(relations, tile_mask.shape[1], blocks), sub_rows, axis=2
        )
        edges = expand_edges(packed_all, flags_all)
        degree = jnp.sum(edges, axis=(0, 2)).astype(jnp.float32).reshape(rels, sub_rows)
        edges = edges.astype(jnp.bfloat16)

        def scatter_sum(parts):
            total = lax.dynamic_index_in_dim(parts, j, 0, keepdims=False).astype(jnp.float32)
            for s in range(1, rels):
                part = lax.dynamic_index_in_dim(parts, (j + s) % rels, 0, keepdims=False)
                total = total + from_shift(part, "rel", rels, s).astype(jnp.float32)
            return total

        shared, (edges, degree, weight_own) = gather_pairs(
            others, blks, group, (edges, degree, weight_own)
        )
        pieces = [got for _, got in shared]
        if piece % 16:
            rest = jnp.zeros((rels - 1, blks, piece, cols), jnp.bfloat16)
            for source, got in shared:
                rest = lax.dynamic_update_index_in_dim(rest, got, source, 1)
            pieces = [rest.reshape(rels - 1, rows, cols)]
        message, own = messages(
            jnp.stack([source for source, _ in gathered]).astype(jnp.int32),
            ordered, [got for _, got in gathered], weight_own, pieces, edges,
        )
        message, degree = lax.optimization_barrier((message, degree))
        degree = scatter_sum(degree)
        message = scatter_sum(message.reshape(rels, sub_rows, width))
        return jax.nn.relu(own + message * lax.rsqrt(1.0 + degree)[:, None]).astype(jnp.bfloat16)

    return shards


def solution(mesh):
    placed = (
        P(("blk", "rel"), None),
        P(None, "blk", "rel", None),
        P(None, "blk", None, "rel"),
        P("rel", None, None),
        P(),
        P("rel", None),
    )
    return jax.shard_map(
        make(mesh.shape["blk"], mesh.shape["rel"]), mesh=mesh, in_specs=placed,
        out_specs=P(("blk", "rel"), None), check_vma=False,
    )
```
